32 devices in a mesh: rows: 4 (over x, core), vocab: 8 (over z, y).
Axes of the slice: x: 2, y: 2, z: 4, core: 2. Of those that a mesh axis runs over, the one named last changes fastest.
Arguments:
- draft_hidden: bfloat16 [2048, 2048], P('rows'), may hold values from -128 to 128
- teacher_hidden: bfloat16 [2048, 8192], P('rows'), may hold values from -128 to 128
- draft_head: bfloat16 [2048, 8192], P(None, 'vocab'), may hold values from -4 to 4
- teacher_head: bfloat16 [8192, 8192], P(None, ('vocab', 'rows')), may hold values from -4 to 4
- row_weight: float32 [2048], P('rows'), may hold values from 1 to 16
Outputs:
- grad_hidden: bfloat16 [2048, 2048], P('rows')
- grad_head: bfloat16 [2048, 8192], P('rows', 'vocab')
- kl_rows: float32 [2048], P('rows')
The draws below stay inside these ranges and needn't reach their ends.
All inputs are finite; a program needn't handle non-finite values.
Results may differ from the reference program's by a relative error of at most 0.0051.
Values may be sent and summed in bfloat16 or wider, within the bound.
A program may use at most 192 MiB of HBM per device.

```python
import math
import jax
import jax.numpy as jnp

D_DRAFT = 2048
D_TEACH = 8192
TOKENS = 2048
VOCAB = 8192


def make_pair(key, salt, width, spread):
    folded = jax.random.fold_in(key, salt)
    key_weight, key_state = jax.random.split(folded, 2)
    weight = spread * jnp.clip(jax.random.normal(key_weight, (width, VOCAB), jnp.float32), -6.0, 6.0)
    states = jnp.clip(jax.random.normal(key_state, (TOKENS, width), jnp.float32), -6.0, 6.0)
    return (weight, states)


def draw_draft_hidden(key, part):
    return make_pair(key, 11, D_DRAFT, 3.5 / D_DRAFT ** 0.5)[1].astype(jnp.bfloat16)


def draw_draft_head(key, part):
    return make_pair(key, 11, D_DRAFT, 3.5 / D_DRAFT ** 0.5)[0].astype(jnp.bfloat16)


def draw_teacher_hidden(key, part):
    return make_pair(key, 23, D_TEACH, 4.0 / D_TEACH ** 0.5)[1].astype(jnp.bfloat16)


def draw_teacher_head(key, part):
    return make_pair(key, 23, D_TEACH, 4.0 / D_TEACH ** 0.5)[0].astype(jnp.bfloat16)


def steps_of(own_key, shape, cuts, low, top_value):
    loudness = 1.0
    for dim, blocks in cuts:
        draws = jax.random.uniform(jax.random.fold_in(jax.random.fold_in(own_key, 6), dim), (blocks,), jnp.float32, low / len(cuts), top_value / len(cuts))
        loudness = loudness * jnp.repeat(jnp.exp(draws), shape[dim] // blocks).reshape((-1,) + (1,) * (len(shape) - 1 - dim))
    return loudness


def setup_inputs(seed: int = 0) -> dict:
    key_list = jax.random.split(jax.random.key(seed), 6)
    draft_hidden = draw_draft_hidden(jax.random.fold_in(key_list[5], 71), 0)
    teacher_hidden = draw_teacher_hidden(jax.random.fold_in(key_list[5], 71), 0)
    draft_head = draw_draft_head(jax.random.fold_in(key_list[5], 71), 0)
    teacher_head = draw_teacher_head(jax.random.fold_in(key_list[5], 71), 0)
    row_weight = jnp.clip(jnp.exp(math.log(16.0) - 2.7725887 * jax.random.uniform(key_list[4], (TOKENS,), jnp.float32) ** steps_of(key_list[4], (TOKENS,), ((0, 4),), -0.2, 0.2)), 1.0, 16.0)
    return {"draft_hidden": draft_hidden, "teacher_hidden": teacher_hidden, "draft_head": draft_head, "teacher_head": teacher_head, "row_weight": row_weight}


def log_total(logits):
    peak = jnp.max(logits, axis=1)
    return peak + jnp.log(jnp.sum(jnp.exp(logits - peak[:, None]), axis=1))


def reference(draft_hidden, teacher_hidden, draft_head, teacher_head, row_weight):
    draft_logits = jnp.dot(draft_hidden, draft_head, preferred_element_type=jnp.float32)
    teacher_logits = jnp.dot(teacher_hidden, teacher_head, preferred_element_type=jnp.float32)
    draft_lse = log_total(draft_logits)
    teacher_lse = log_total(teacher_logits)
    teacher_prob = jnp.exp(teacher_logits - teacher_lse[:, None])
    draft_prob = jnp.exp(draft_logits - draft_lse[:, None])
    kl_rows = row_weight * (jnp.sum(teacher_prob * (teacher_logits - draft_logits), axis=1) - teacher_lse + draft_lse)
    grad_logits = (row_weight[:, None] * (draft_prob - teacher_prob)).astype(jnp.bfloat16)
    grad_hidden = jnp.dot(grad_logits, draft_head.T, preferred_element_type=jnp.float32).astype(jnp.bfloat16)
    grad_head = jnp.dot(draft_hidden.T, grad_logits, preferred_element_type=jnp.float32).astype(jnp.bfloat16)
    return grad_hidden, grad_head, kl_rows
```

```python
import jax
import jax.numpy as jnp
from jax import lax
from jax.sharding import PartitionSpec as P


F32, BF16 = jnp.float32, jnp.bfloat16


def make(rows, vocab):
    cores = 2 if rows % 2 == 0 else 1
    nx = rows // cores
    ny = nx if vocab % nx == 0 else 1
    nz = vocab // ny

    def shift(array, axis, dx=0, dc=0, dy=0, dz=0):
        if axis == "rows":
            perm = [
                (x * cores + c, (x + dx) % nx * cores + (c + dc) % cores)
                for x in range(nx)
                for c in range(cores)
            ]
        else:
            perm = [
                (z * ny + y, (z + dz) % nz * ny + (y + dy) % ny)
                for z in range(nz)
                for y in range(ny)
            ]
        return lax.ppermute(array, axis, perm)

    def dot(a, b):
        return jnp.dot(a, b, preferred_element_type=F32)

    def teacher(hidden, head, row):
        x, core = row // cores, row % cores
        width = head.shape[1]
        pieces = 4
        depth = head.shape[0] // pieces
        total = {}
        for dc in range(cores):
            total[0, dc] = dot(hidden, shift(head, "rows", dc=dc) if dc else head)
        held = [head[k * depth : (k + 1) * depth] for k in range(pieces)]
        for dx in range(1, nx):
            held = [shift(h, "rows", dx=1) for h in held]
            for k in range(pieces):
                part = hidden[:, k * depth : (k + 1) * depth]
                for dc in range(cores):
                    piece = shift(held[k], "rows", dc=dc) if dc else held[k]
                    term = dot(part, piece)
                    total[dx, dc] = total[dx, dc] + term if k else term
        out = jnp.zeros((hidden.shape[0], width * rows), F32)
        for (dx, dc), block in total.items():
            owner = (x + nx - dx) % nx * cores + (core + cores - dc) % cores
            out = lax.dynamic_update_slice(out, block, (0, owner * width))
        return out

    def sum_hidden(grad_logits, draft_head, vocab_id):
        y, z = vocab_id % ny, vocab_id // ny
        tokens = grad_logits.shape[0]
        chunks = 4
        size = tokens // chunks
        outs = []
        for i in range(chunks):
            part = lax.dot_general(
                grad_logits[i * size : (i + 1) * size],
                draft_head,
                (((1,), (1,)), ((), ())),
                preferred_element_type=F32,
            )
            step = size // ny
            take = lambda a, i, n: lax.dynamic_slice_in_dim(a, i * n, n, 0)
            mine = take(part, y, step)
            for d in range(1, ny):
                mine = mine + shift(take(part, (y + d) % ny, step).astype(BF16), "vocab", dy=d).astype(F32)
            small = step // nz
            own = take(mine, z, small)
            for d in range(1, nz):
                own = own + shift(take(mine, (z + d) % nz, small).astype(BF16), "vocab", dz=d).astype(F32)
            own = own.astype(BF16)
            out = jnp.zeros((step, part.shape[1]), BF16)
            for d in range(nz):
                got = shift(own, "vocab", dz=d) if d else own
                out = lax.dynamic_update_slice(out, got, ((z + nz - d) % nz * small, 0))
            full = jnp.zeros((size, part.shape[1]), BF16)
            for d in range(ny):
                got = shift(out, "vocab", dy=d) if d else out
                full = lax.dynamic_update_slice(full, got, ((y + ny - d) % ny * step, 0))
            outs.append(full)
        return jnp.concatenate(outs, axis=0)

    def sum_head(draft_hidden, grad_logits, row):
        x, core = row // cores, row % cores
        part = lax.dot_general(
            draft_hidden, grad_logits, (((0,), (0,)), ((), ())), preferred_element_type=F32
        )
        part = part.reshape(nx, cores, part.shape[0] // rows, part.shape[1])
        take = lambda a, i, dim: lax.dynamic_index_in_dim(a, i, dim, keepdims=False)
        mine = take(part, core, 1)
        for d in range(1, cores):
            mine = mine + shift(take(part, (core + d) % cores, 1).astype(BF16), "rows", dc=d).astype(F32)
        own = take(mine, x, 0)
        for d in range(1, nx):
            own = own + shift(take(mine, (x + d) % nx, 0).astype(BF16), "rows", dx=d).astype(F32)
        return own.astype(BF16)

    def on_device(draft_hidden, teacher_hidden, draft_head, teacher_head, row_weight):
        row, vocab_id = lax.axis_index("rows"), lax.axis_index("vocab")
        draft_logits = dot(draft_hidden, draft_head)
        teacher_logits = teacher(teacher_hidden, teacher_head, row)
        draft_top = jnp.max(draft_logits, axis=1)
        teach_top = jnp.max(teacher_logits, axis=1)
        teach_exp = jnp.exp(teacher_logits - teach_top[:, None])
        stats = jnp.stack(
            [
                draft_top,
                teach_top,
                jnp.sum(jnp.exp(draft_logits - draft_top[:, None]), axis=1),
                jnp.sum(teach_exp, axis=1),
                jnp.sum(teach_exp * (teacher_logits - draft_logits), axis=1),
            ]
        )
        stats = lax.all_gather(stats, "vocab", axis=0)
        draft_top, teach_top = jnp.max(stats[:, 0], axis=0), jnp.max(stats[:, 1], axis=0)
        draft_scale = jnp.exp(stats[:, 0] - draft_top)
        teach_scale = jnp.exp(stats[:, 1] - teach_top)
        draft_sum = jnp.sum(stats[:, 2] * draft_scale, axis=0)
        teach_sum = jnp.sum(stats[:, 3] * teach_scale, axis=0)
        teach_gap = jnp.sum(stats[:, 4] * teach_scale, axis=0)
        draft_lse = draft_top + jnp.log(draft_sum)
        teacher_lse = teach_top + jnp.log(teach_sum)
        kl_rows = row_weight * (teach_gap / teach_sum - teacher_lse + draft_lse)
        teacher_prob = jnp.exp(teacher_logits - teacher_lse[:, None])
        draft_prob = jnp.exp(draft_logits - draft_lse[:, None])
        grad_logits = (row_weight[:, None] * (draft_prob - teacher_prob)).astype(BF16)
        grad_hidden = sum_hidden(grad_logits, draft_head, vocab_id)
        grad_head = sum_head(draft_hidden, grad_logits, row)
        return (grad_hidden, grad_head, kl_rows)

    return on_device


def solution(mesh):
    return jax.shard_map(
        make(mesh.shape["rows"], mesh.shape["vocab"]),
        mesh=mesh,
        in_specs=(
            P("rows", None),
            P("rows", None),
            P(None, "vocab"),
            P(None, ("vocab", "rows")),
            P("rows"),
        ),
        out_specs=(P("rows", None), P("rows", "vocab"), P("rows")),
        check_vma=False,
    )
```

```python
import jax
import jax.numpy as jnp
from jax import lax
from jax.experimental import pallas as pl
from jax.experimental.pallas import tpu as pltpu
from jax.sharding import PartitionSpec as P


F32, BF16 = jnp.float32, jnp.bfloat16


def make(rows, vocab):
    cores = 2 if rows % 2 == 0 else 1
    nx = rows // cores
    ny = nx if vocab % nx == 0 else 1
    nz = vocab // ny

    def shift(array, axis, dx=0, dc=0, dy=0, dz=0):
        if axis == "rows":
            perm = [
                (x * cores + c, (x + dx) % nx * cores + (c + dc) % cores)
                for x in range(nx)
                for c in range(cores)
            ]
        else:
            perm = [
                (z * ny + y, (z + dz) % nz * ny + (y + dy) % ny)
                for z in range(nz)
                for y in range(ny)
            ]
        return lax.ppermute(array, axis, perm)

    def dot(a, b):
        return jnp.dot(a, b, preferred_element_type=F32)

    def teacher(hidden, head, row, early):
        x, core = row // cores, row % cores
        width = head.shape[1]
        pieces = 4
        depth = head.shape[0] // pieces
        total = {}
        for dc in range(cores):
            total[0, dc] = dot(hidden, shift(head, "rows", dc=dc) if dc else head)
        held = [head[k * depth : (k + 1) * depth] for k in range(pieces)]
        for dx in range(1, nx):
            held = [shift(h, "rows", dx=1) for h in held]
            if dx == 1:
                held[pieces // 2], total, early = lax.optimization_barrier(
                    (held[pieces // 2], total, early)
                )
            for k in range(pieces):
                part = hidden[:, k * depth : (k + 1) * depth]
                for dc in range(cores):
                    piece = shift(held[k], "rows", dc=dc) if dc else held[k]
                    term = dot(part, piece)
                    total[dx, dc] = total[dx, dc] + term if k else term
        out = jnp.zeros((hidden.shape[0], width * rows), F32)
        for (dx, dc), block in total.items():
            owner = (x + nx - dx) % nx * cores + (core + cores - dc) % cores
            out = lax.dynamic_update_slice(out, block, (0, owner * width))
        return out, early

    def greet(peers):
        barrier = pltpu.get_barrier_semaphore()
        for peer in peers:
            pl.semaphore_signal(
                barrier, inc=1, device_id=peer, device_id_type=pl.DeviceIdType.MESH
            )
        pl.semaphore_wait(barrier, len(peers))

    def swap_stats(stats):
        def kernel(x_ref, out_ref, send_sem, recv_sem):
            row, me = lax.axis_index("rows"), lax.axis_index("vocab")
            peers = [(row, lax.rem(me + d, vocab)) for d in range(1, vocab)]
            greet(peers)
            copies = []
            for d, peer in enumerate(peers):
                copy = pltpu.make_async_remote_copy(
                    src_ref=x_ref,
                    dst_ref=out_ref.at[me],
                    send_sem=send_sem.at[d],
                    recv_sem=recv_sem.at[d],
                    device_id=peer,
                    device_id_type=pl.DeviceIdType.MESH,
                )
                copy.start()
                copies.append(copy)
            out_ref[me] = x_ref[...]
            for copy in copies:
                copy.wait()

        return pl.pallas_call(
            kernel,
            out_shape=jax.ShapeDtypeStruct((vocab,) + stats.shape, F32),
            in_specs=[pl.BlockSpec(memory_space=pltpu.VMEM)],
            out_specs=pl.BlockSpec(memory_space=pltpu.VMEM),
            scratch_shapes=[
                pltpu.SemaphoreType.DMA((vocab - 1,)),
                pltpu.SemaphoreType.DMA((vocab - 1,)),
            ],
            compiler_params=pltpu.CompilerParams(collective_id=0, has_side_effects=True),
        )(stats)

    def sums(grad_logits, draft_head, hidden_t):
        tokens, width = grad_logits.shape
        draft = draft_head.shape[0]
        chunks = 4
        cols, ry = draft // chunks, tokens // ny
        rz, block = ry // nz, draft // rows

        def kernel(
            gl, w, ht, out, head_out,
            ysend, yrecv, acc, zsend, zrecv, csend, crecv, hacc, xsend, xrecv,
            y1s, y1r, z1s, z1r, z2s, z2r, y2s, y2r, cs, cr, xs, xr,
        ):
            row, me = lax.axis_index("rows"), lax.axis_index("vocab")
            x, core = row // cores, lax.rem(row, cores)
            z, y = me // ny, lax.rem(me, ny)
            ypeers = [(row, z * ny + lax.rem(y + d, ny)) for d in range(1, ny)]
            zpeers = [(row, lax.rem(z + d, nz) * ny + y) for d in range(1, nz)]
            cpeers = [(x * cores + lax.rem(core + d, cores), me) for d in range(1, cores)]
            xpeers = [(lax.rem(x + d, nx) * cores + core, me) for d in range(1, nx)]

            def remote(src, dst, s, r, peer):
                return pltpu.make_async_remote_copy(
                    src_ref=src, dst_ref=dst, send_sem=s, recv_sem=r,
                    device_id=peer, device_id_type=pl.DeviceIdType.MESH,
                )

            def al(v, n):
                return pl.multiple_of(v * n, n)

            def y1(d, i):
                return remote(ysend.at[d, i], yrecv.at[d, i], y1s.at[d, i], y1r.at[d, i], ypeers[d])

            def z1(d, i):
                return remote(zsend.at[d, i], zrecv.at[d, i], z1s.at[d, i], z1r.at[d, i], zpeers[d])

            def z2(d, i):
                ref = out.at[pl.ds(al(y * nz + z, rz), rz), pl.ds(i * cols, cols)]
                return remote(ref, ref, z2s.at[d, i], z2r.at[d, i], zpeers[d])

            def y2(d, i):
                ref = out.at[pl.ds(al(y, ry), ry), pl.ds(i * cols, cols)]
                return remote(ref, ref, y2s.at[d, i], y2r.at[d, i], ypeers[d])

            def cx(d, k):
                return remote(csend.at[d, k], crecv.at[d, k], cs.at[d, k], cr.at[d, k], cpeers[d])

            def xx(d):
                return remote(xsend.at[d], xrecv.at[d], xs.at[d], xr.at[d], xpeers[d])

            def hidden_dot(part, i):
                return lax.dot_general(
                    gl[pl.ds(al(part, ry), ry), :],
                    w[pl.ds(al(i, cols), cols), :],
                    (((1,), (1,)), ((), ())),
                    preferred_element_type=F32,
                )

            def head_dot(part):
                return jnp.dot(
                    ht[pl.ds(al(part, block), block), :], gl[...], preferred_element_type=F32
                )

            greet(ypeers + zpeers + cpeers + xpeers)

            def first(i, carry):
                for d in range(ny - 1):
                    ysend[d, i] = hidden_dot(lax.rem(y + d + 1, ny), i).astype(BF16)
                    y1(d, i).start()
                return carry

            lax.fori_loop(0, chunks, first, 0)

            def core_part(k, carry):
                to = lax.rem(x + k + 1, nx) * cores
                for d in range(cores - 1):
                    csend[d, k] = head_dot(to + lax.rem(core + d + 1, cores)).astype(BF16)
                    cx(d, k).start()
                return carry

            lax.fori_loop(0, nx, core_part, 0)

            def own_part(i, carry):
                acc[i] = hidden_dot(y, i)
                return carry

            lax.fori_loop(0, chunks, own_part, 0)

            def own_head(k, carry):
                hacc[k] = head_dot(lax.rem(x + k + 1, nx) * cores + core)
                return carry

            lax.fori_loop(0, nx, own_head, 0)

            def head_mid():
                for k in range(nx):
                    total = hacc[k]
                    for d in range(cores - 1):
                        cx(d, k).wait_recv()
                        total = total + crecv[d, k].astype(F32)
                    if k < nx - 1:
                        xsend[k] = total.astype(BF16)
                        xx(k).start()
                    else:
                        hacc[k] = total

            def head_end():
                total = hacc[nx - 1]
                for d in range(nx - 1):
                    xx(d).wait_recv()
                    total = total + xrecv[d].astype(F32)
                head_out[...] = total.astype(BF16)

            def stage_a(i):
                for d in range(ny - 1):
                    y1(d, i).wait_recv()
                    acc[i] = acc[i] + yrecv[d, i].astype(F32)
                for d in range(nz - 1):
                    to = lax.rem(z + d + 1, nz)
                    zsend[d, i] = acc[i, pl.ds(al(to, rz), rz), :].astype(BF16)
                    z1(d, i).start()

            def stage_b(i):
                total = acc[i, pl.ds(al(z, rz), rz), :]
                for d in range(nz - 1):
                    z1(d, i).wait_recv()
                    total = total + zrecv[d, i].astype(F32)
                out[pl.ds(al(y * nz + z, rz), rz), i * cols : (i + 1) * cols] = total.astype(BF16)
                for d in range(nz - 1):
                    z2(d, i).start()

            def stage_c(i):
                for d in range(nz - 1):
                    z2(d, i).wait_recv()
                for d in range(ny - 1):
                    y2(d, i).start()

            head_mid()
            for step in range(chunks + 2):
                if step < chunks:
                    stage_a(step)
                if 1 <= step <= chunks:
                    stage_b(step - 1)
                if step >= 2:
                    stage_c(step - 2)
            head_end()
            for i in range(chunks):
                for d in range(ny - 1):
                    y2(d, i).wait_recv()
                    y1(d, i).wait_send()
                    y2(d, i).wait_send()
                for d in range(nz - 1):
                    z1(d, i).wait_send()
                    z2(d, i).wait_send()
            for k in range(nx):
                for d in range(cores - 1):
                    cx(d, k).wait_send()
            for d in range(nx - 1):
                xx(d).wait_send()

        def dma(*shape):
            return pltpu.SemaphoreType.DMA(tuple(max(n, 1) for n in shape))

        def vm(dtype, *shape):
            return pltpu.VMEM(tuple(max(n, 1) for n in shape), dtype)

        return pl.pallas_call(
            kernel,
            out_shape=(
                jax.ShapeDtypeStruct((tokens, draft), BF16),
                jax.ShapeDtypeStruct((block, width), BF16),
            ),
            in_specs=[pl.BlockSpec(memory_space=pltpu.VMEM)] * 3,
            out_specs=(pl.BlockSpec(memory_space=pltpu.VMEM),) * 2,
            scratch_shapes=[
                vm(BF16, ny - 1, chunks, ry, cols),
                vm(BF16, ny - 1, chunks, ry, cols),
                vm(F32, chunks, ry, cols),
                vm(BF16, nz - 1, chunks, rz, cols),
                vm(BF16, nz - 1, chunks, rz, cols),
                vm(BF16, cores - 1, nx, block, width),
                vm(BF16, cores - 1, nx, block, width),
                vm(F32, nx, block, width),
                vm(BF16, nx - 1, block, width),
                vm(BF16, nx - 1, block, width),
            ]
            + [dma(ny - 1, chunks)] * 2
            + [dma(nz - 1, chunks)] * 4
            + [dma(ny - 1, chunks)] * 2
            + [dma(cores - 1, nx)] * 2
            + [dma(nx - 1)] * 2,
            compiler_params=pltpu.CompilerParams(
                collective_id=1, has_side_effects=True, vmem_limit_bytes=56 * 1024 * 1024
            ),
        )(grad_logits, draft_head, hidden_t)

    def on_device(draft_hidden, teacher_hidden, draft_head, teacher_head, row_weight):
        row = lax.axis_index("rows")
        draft_logits = dot(draft_hidden, draft_head)
        draft_top = jnp.max(draft_logits, axis=1)
        draft_sum = jnp.sum(jnp.exp(draft_logits - draft_top[:, None]), axis=1)
        early = (draft_logits, draft_top, draft_sum, draft_hidden.T)
        teacher_logits, early = teacher(teacher_hidden, teacher_head, row, early)
        draft_logits, draft_top, draft_sum, hidden_t = early
        teach_top = jnp.max(teacher_logits, axis=1)
        teach_exp = jnp.exp(teacher_logits - teach_top[:, None])
        stats = jnp.stack(
            [
                draft_top,
                teach_top,
                draft_sum,
                jnp.sum(teach_exp, axis=1),
                jnp.sum(teach_exp * (teacher_logits - draft_logits), axis=1),
            ]
        )
        stats = swap_stats(stats)
        draft_top, teach_top = jnp.max(stats[:, 0], axis=0), jnp.max(stats[:, 1], axis=0)
        draft_scale = jnp.exp(stats[:, 0] - draft_top)
        teach_scale = jnp.exp(stats[:, 1] - teach_top)
        draft_sum = jnp.sum(stats[:, 2] * draft_scale, axis=0)
        teach_sum = jnp.sum(stats[:, 3] * teach_scale, axis=0)
        teach_gap = jnp.sum(stats[:, 4] * teach_scale, axis=0)
        draft_lse = draft_top + jnp.log(draft_sum)
        teacher_lse = teach_top + jnp.log(teach_sum)
        kl_rows = row_weight * (teach_gap / teach_sum - teacher_lse + draft_lse)
        teacher_prob = jnp.exp(teacher_logits - teacher_lse[:, None])
        draft_prob = jnp.exp(draft_logits - draft_lse[:, None])
        grad_logits = (row_weight[:, None] * (draft_prob - teacher_prob)).astype(BF16)
        grad_hidden, grad_head = sums(grad_logits, draft_head, hidden_t)
        return (grad_hidden, grad_head, kl_rows)

    return on_device


def solution(mesh):
    return jax.shard_map(
        make(mesh.shape["rows"], mesh.shape["vocab"]),
        mesh=mesh,
        in_specs=(
            P("rows", None),
            P("rows", None),
            P(None, "vocab"),
            P(None, ("vocab", "rows")),
            P("rows"),
        ),
        out_specs=(P("rows", None), P("rows", "vocab"), P("rows")),
        check_vma=False,
    )
```

```python
import jax
import jax.numpy as jnp
from jax import lax
from jax.experimental import pallas as pl
from jax.experimental.pallas import tpu as pltpu
from jax.sharding import PartitionSpec as P


F32, BF16 = jnp.float32, jnp.bfloat16


def make(rows, vocab):
    cores = 2 if rows % 2 == 0 else 1
    nx = rows // cores
    ny = nx if vocab % nx == 0 else 1
    nz = vocab // ny

    def shift(array, axis, dx=0, dc=0, dy=0, dz=0):
        if axis == "rows":
            perm = [
                (x * cores + c, (x + dx) % nx * cores + (c + dc) % cores)
                for x in range(nx)
                for c in range(cores)
            ]
        else:
            perm = [
                (z * ny + y, (z + dz) % nz * ny + (y + dy) % ny)
                for z in range(nz)
                for y in range(ny)
            ]
        return lax.ppermute(array, axis, perm)

    def dot(a, b):
        return jnp.dot(a, b, preferred_element_type=F32)

    def teacher(hidden, head, row, early):
        x, core = row // cores, row % cores
        width = head.shape[1]
        unit = head.shape[0] // 4
        cuts = [(k * unit, (k + 1) * unit) for k in range(4)]
        total = {}
        for dc in range(cores):
            total[0, dc] = dot(hidden, shift(head, "rows", dc=dc) if dc else head)
        held = [head[lo:hi] for lo, hi in cuts]
        for dx in range(1, nx):
            held = [shift(h, "rows", dx=1) for h in held]
            for k, (lo, hi) in enumerate(cuts):
                if k in (0, len(cuts) - 1):
                    held[k], total, early = lax.optimization_barrier((held[k], total, early))
                part = hidden[:, lo:hi]
                for dc in range(cores):
                    piece = shift(held[k], "rows", dc=dc) if dc else held[k]
                    term = dot(part, piece)
                    total[dx, dc] = total[dx, dc] + term if k else term
        out = jnp.zeros((hidden.shape[0], width * rows), F32)
        for (dx, dc), block in total.items():
            owner = (x + nx - dx) % nx * cores + (core + cores - dc) % cores
            out = lax.dynamic_update_slice(out, block, (0, owner * width))
        return out, early

    def greet(peers):
        barrier = pltpu.get_barrier_semaphore()
        for peer in peers:
            pl.semaphore_signal(
                barrier, inc=1, device_id=peer, device_id_type=pl.DeviceIdType.MESH
            )
        pl.semaphore_wait(barrier, len(peers))

    def swap_stats(stats):
        def kernel(x_ref, out_ref, send_sem, recv_sem):
            row, me = lax.axis_index("rows"), lax.axis_index("vocab")
            peers = [(row, lax.rem(me + d, vocab)) for d in range(1, vocab)]
            greet(peers)
            copies = []
            for d, peer in enumerate(peers):
                copy = pltpu.make_async_remote_copy(
                    src_ref=x_ref,
                    dst_ref=out_ref.at[me],
                    send_sem=send_sem.at[d],
                    recv_sem=recv_sem.at[d],
                    device_id=peer,
                    device_id_type=pl.DeviceIdType.MESH,
                )
                copy.start()
                copies.append(copy)
            out_ref[me] = x_ref[...]
            for copy in copies:
                copy.wait()

        return pl.pallas_call(
            kernel,
            out_shape=jax.ShapeDtypeStruct((vocab,) + stats.shape, F32),
            in_specs=[pl.BlockSpec(memory_space=pltpu.VMEM)],
            out_specs=pl.BlockSpec(memory_space=pltpu.VMEM),
            scratch_shapes=[
                pltpu.SemaphoreType.DMA((vocab - 1,)),
                pltpu.SemaphoreType.DMA((vocab - 1,)),
            ],
            compiler_params=pltpu.CompilerParams(collective_id=0, has_side_effects=True),
        )(stats)

    def sums(grad_logits, draft_head, hidden_t):
        tokens, width = grad_logits.shape
        draft = draft_head.shape[0]
        chunks = 8
        cols, ry = draft // chunks, tokens // ny
        rz, block = ry // nz, draft // rows

        def kernel(
            gl, w, ht, out, head_out,
            ysend, yrecv, acc, zsend, zrecv, csend, crecv, hacc, xsend, xrecv,
            y1s, y1r, z1s, z1r, z2s, z2r, y2s, y2r, cs, cr, xs, xr,
        ):
            row, me = lax.axis_index("rows"), lax.axis_index("vocab")
            x, core = row // cores, lax.rem(row, cores)
            z, y = me // ny, lax.rem(me, ny)
            ypeers = [(row, z * ny + lax.rem(y + d, ny)) for d in range(1, ny)]
            zpeers = [(row, lax.rem(z + d, nz) * ny + y) for d in range(1, nz)]
            cpeers = [(x * cores + lax.rem(core + d, cores), me) for d in range(1, cores)]
            xpeers = [(lax.rem(x + d, nx) * cores + core, me) for d in range(1, nx)]

            def remote(src, dst, s, r, peer):
                return pltpu.make_async_remote_copy(
                    src_ref=src, dst_ref=dst, send_sem=s, recv_sem=r,
                    device_id=peer, device_id_type=pl.DeviceIdType.MESH,
                )

            def al(v, n):
                return pl.multiple_of(v * n, n)

            def y1(d, i):
                return remote(ysend.at[d, i], yrecv.at[d, i], y1s.at[d, i], y1r.at[d, i], ypeers[d])

            def z1(d, i):
                return remote(zsend.at[d, i], zrecv.at[d, i], z1s.at[d, i], z1r.at[d, i], zpeers[d])

            def z2(d, i):
                ref = out.at[pl.ds(al(y * nz + z, rz), rz), pl.ds(i * cols, cols)]
                return remote(ref, ref, z2s.at[d, i], z2r.at[d, i], zpeers[d])

            def y2(d, i):
                ref = out.at[pl.ds(al(y, ry), ry), pl.ds(i * cols, cols)]
                return remote(ref, ref, y2s.at[d, i], y2r.at[d, i], ypeers[d])

            def cx(d, k):
                return remote(csend.at[d, k], crecv.at[d, k], cs.at[d, k], cr.at[d, k], cpeers[d])

            def xx(d):
                return remote(xsend.at[d], xrecv.at[d], xs.at[d], xr.at[d], xpeers[d])

            def hidden_dot(part, i):
                return lax.dot_general(
                    gl[pl.ds(al(part, ry), ry), :],
                    w[pl.ds(al(i, cols), cols), :],
                    (((1,), (1,)), ((), ())),
                    preferred_element_type=F32,
                )

            def head_dot(part):
                return jnp.dot(
                    ht[pl.ds(al(part, block), block), :], gl[...], preferred_element_type=F32
                )

            greet(ypeers + zpeers + cpeers + xpeers)

            def first(i, carry):
                for d in range(ny - 1):
                    ysend[d, i] = hidden_dot(lax.rem(y + d + 1, ny), i).astype(BF16)
                    y1(d, i).start()
                return carry

            def own_part(i, carry):
                acc[i] = hidden_dot(y, i)
                return carry

            lax.fori_loop(0, chunks, first, 0)
            lax.fori_loop(0, chunks, own_part, 0)

            def core_part(k, carry):
                to = lax.rem(x + k + 1, nx) * cores
                for d in range(cores - 1):
                    csend[d, k] = head_dot(to + lax.rem(core + d + 1, cores)).astype(BF16)
                    cx(d, k).start()
                return carry

            lax.fori_loop(0, nx, core_part, 0)

            def own_head(k, carry):
                hacc[k] = head_dot(lax.rem(x + k + 1, nx) * cores + core)
                return carry

            def head_mid():
                for k in range(nx):
                    total = hacc[k]
                    for d in range(cores - 1):
                        cx(d, k).wait_recv()
                        total = total + crecv[d, k].astype(F32)
                    if k < nx - 1:
                        xsend[k] = total.astype(BF16)
                        xx(k).start()
                    else:
                        hacc[k] = total

            def head_end():
                total = hacc[nx - 1]
                for d in range(nx - 1):
                    xx(d).wait_recv()
                    total = total + xrecv[d].astype(F32)
                head_out[...] = total.astype(BF16)

            def stage_a(i):
                for d in range(ny - 1):
                    y1(d, i).wait_recv()
                    acc[i] = acc[i] + yrecv[d, i].astype(F32)
                for d in range(nz - 1):
                    to = lax.rem(z + d + 1, nz)
                    zsend[d, i] = acc[i, pl.ds(al(to, rz), rz), :].astype(BF16)
                    z1(d, i).start()

            def stage_b(i):
                total = acc[i, pl.ds(al(z, rz), rz), :]
                for d in range(nz - 1):
                    z1(d, i).wait_recv()
                    total = total + zrecv[d, i].astype(F32)
                out[pl.ds(al(y * nz + z, rz), rz), i * cols : (i + 1) * cols] = total.astype(BF16)
                for d in range(nz - 1):
                    z2(d, i).start()

            def stage_c(i):
                for d in range(nz - 1):
                    z2(d, i).wait_recv()
                for d in range(ny - 1):
                    y2(d, i).start()

            for step in range(chunks + 2):
                if step < chunks:
                    stage_a(step)
                if step == 0:
                    lax.fori_loop(0, nx, own_head, 0)
                    head_mid()
                if 1 <= step <= chunks:
                    stage_b(step - 1)
                if step >= 2:
                    stage_c(step - 2)
            head_end()
            for i in range(chunks):
                for d in range(ny - 1):
                    y2(d, i).wait_recv()
                    y1(d, i).wait_send()
                    y2(d, i).wait_send()
                for d in range(nz - 1):
                    z1(d, i).wait_send()
                    z2(d, i).wait_send()
            for k in range(nx):
                for d in range(cores - 1):
                    cx(d, k).wait_send()
            for d in range(nx - 1):
                xx(d).wait_send()

        def dma(*shape):
            return pltpu.SemaphoreType.DMA(tuple(max(n, 1) for n in shape))

        def vm(dtype, *shape):
            return pltpu.VMEM(tuple(max(n, 1) for n in shape), dtype)

        return pl.pallas_call(
            kernel,
            out_shape=(
                jax.ShapeDtypeStruct((tokens, draft), BF16),
                jax.ShapeDtypeStruct((block, width), BF16),
            ),
            in_specs=[pl.BlockSpec(memory_space=pltpu.VMEM)] * 3,
            out_specs=(pl.BlockSpec(memory_space=pltpu.VMEM),) * 2,
            scratch_shapes=[
                vm(BF16, ny - 1, chunks, ry, cols),
                vm(BF16, ny - 1, chunks, ry, cols),
                vm(F32, chunks, ry, cols),
                vm(BF16, nz - 1, chunks, rz, cols),
                vm(BF16, nz - 1, chunks, rz, cols),
                vm(BF16, cores - 1, nx, block, width),
                vm(BF16, cores - 1, nx, block, width),
                vm(F32, nx, block, width),
                vm(BF16, nx - 1, block, width),
                vm(BF16, nx - 1, block, width),
            ]
            + [dma(ny - 1, chunks)] * 2
            + [dma(nz - 1, chunks)] * 4
            + [dma(ny - 1, chunks)] * 2
            + [dma(cores - 1, nx)] * 2
            + [dma(nx - 1)] * 2,
            compiler_params=pltpu.CompilerParams(
                collective_id=1, has_side_effects=True, vmem_limit_bytes=56 * 1024 * 1024
            ),
        )(grad_logits, draft_head, hidden_t)

    def on_device(draft_hidden, teacher_hidden, draft_head, teacher_head, row_weight):
        row = lax.axis_index("rows")
        draft_logits = dot(draft_hidden, draft_head)
        draft_top = jnp.max(draft_logits, axis=1)
        draft_sum = jnp.sum(jnp.exp(draft_logits - draft_top[:, None]), axis=1)
        early = (draft_logits, draft_top, draft_sum, draft_hidden.T)
        teacher_logits, early = teacher(teacher_hidden, teacher_head, row, early)
        draft_logits, draft_top, draft_sum, hidden_t = early
        teach_top = jnp.max(teacher_logits, axis=1)
        teach_exp = jnp.exp(teacher_logits - teach_top[:, None])
        stats = jnp.stack(
            [
                draft_top,
                teach_top,
                draft_sum,
                jnp.sum(teach_exp, axis=1),
                jnp.sum(teach_exp * (teacher_logits - draft_logits), axis=1),
            ]
        )
        stats = swap_stats(stats)
        draft_top, teach_top = jnp.max(stats[:, 0], axis=0), jnp.max(stats[:, 1], axis=0)
        draft_scale = jnp.exp(stats[:, 0] - draft_top)
        teach_scale = jnp.exp(stats[:, 1] - teach_top)
        draft_sum = jnp.sum(stats[:, 2] * draft_scale, axis=0)
        teach_sum = jnp.sum(stats[:, 3] * teach_scale, axis=0)
        teach_gap = jnp.sum(stats[:, 4] * teach_scale, axis=0)
        draft_lse = draft_top + jnp.log(draft_sum)
        teacher_lse = teach_top + jnp.log(teach_sum)
        kl_rows = row_weight * (teach_gap / teach_sum - teacher_lse + draft_lse)
        teacher_prob = jnp.exp(teacher_logits - teacher_lse[:, None])
        draft_prob = jnp.exp(draft_logits - draft_lse[:, None])
        grad_logits = (row_weight[:, None] * (draft_prob - teacher_prob)).astype(BF16)
        grad_hidden, grad_head = sums(grad_logits, draft_head, hidden_t)
        return (grad_hidden, grad_head, kl_rows)

    return on_device


def solution(mesh):
    return jax.shard_map(
        make(mesh.shape["rows"], mesh.shape["vocab"]),
        mesh=mesh,
        in_specs=(
            P("rows", None),
            P("rows", None),
            P(None, "vocab"),
            P(None, ("vocab", "rows")),
            P("rows"),
        ),
        out_specs=(P("rows", None), P("rows", "vocab"), P("rows")),
        check_vma=False,
    )
```
